256 devices in a mesh: group: 8 (over y, core), member: 32 (over x, z).
Axes of the slice: x: 4, y: 4, z: 8, core: 2. Of those that a mesh axis runs over, the one named last changes fastest.
Arguments:
- leaf_solution: bfloat16 [2048, 64, 128], P(('group', 'member')), may hold values from -6 to 6
- leaf_panels: bfloat16 [2048, 3, 4, 128, 128], P(('group', 'member')), may hold values from -0.09375 to 0.09375
- leaf_rows: int32 [2048, 3, 4], P(('group', 'member')), may hold values from 0 to 127, as said below
- sep_panels: bfloat16 [256, 3, 4, 128, 128], P(('group', 'member')), may hold values from -0.25 to 0.25
- sep_rows: int32 [256, 3, 4], P(('group', 'member')), may hold values from 0 to 127, as said below
- right_sides: bfloat16 [3, 256, 64, 128], P(None, ('group', 'member')), may hold values from -6 to 6
- inverse_low: bfloat16 [256, 4096, 128], P(('group', 'member')), may hold values from -0.09375 to 0.09375
- inverse_mid: bfloat16 [256, 8192, 128], P(('group', 'member')), may hold values from -0.0625 to 0.0625
- inverse_top: bfloat16 [256, 16384, 128], P(('group', 'member')), may hold values from -0.046875 to 0.046875
Outputs:
- solution: bfloat16 [3, 256, 64, 128], P(None, ('group', 'member'))
The draws below stay inside these ranges and needn't reach their ends.
Inputs may be any that keep to these rules, and one draw needn't show every extreme that they name: leaf_rows[k, l, t] is below 32 * 2**l: a block of the ancestor separator at level l; indices may repeat. sep_rows[d, j, t] is below 64, 128, 128 for j = 0, 1, 2: a block of the target separator; indices may repeat.
All inputs are finite; a program needn't handle non-finite values.
Results may differ from the reference program's by a relative error of at most 0.012.
Values may be sent and summed in bfloat16 or wider, within the bound.
No kernel may reach another device: no remote copies, remote signals or barrier semaphores. Data moves between devices by JAX's collectives and lax.ppermute only.
A program may use at most 128 MiB of HBM per device.

```python
import jax
import jax.numpy as jnp
from jax import lax

P_SIZE = 128
R = 64
NT = 4
LB = 8
SEP_BLOCKS = 32
DEV_ALL = 256


def block_indices(key, count, limits):
    raw = jax.random.randint(key, (count, 3, NT), 0, 4 * SEP_BLOCKS, dtype=jnp.int32)
    return raw % jnp.array(limits, dtype=jnp.int32)[None, :, None]


def draw_leaf_rows(key, part):
    return block_indices(jax.random.fold_in(key, 11), DEV_ALL * LB, [SEP_BLOCKS, 2 * SEP_BLOCKS, 4 * SEP_BLOCKS])


def draw_sep_rows(key, part):
    return block_indices(jax.random.fold_in(key, 23), DEV_ALL, [2 * SEP_BLOCKS, 4 * SEP_BLOCKS, 4 * SEP_BLOCKS])


def block_scale(key, shape, split, smallest, top_value):
    def one(axis_at, shards_of):
        draws = jax.random.uniform(jax.random.fold_in(jax.random.fold_in(key, 6), axis_at), (shards_of,), jnp.float32, smallest / len(split), top_value / len(split))
        return jnp.repeat(jnp.exp(draws), shape[axis_at] // shards_of).reshape((-1,) + (1,) * (len(shape) - axis_at - 1))

    gain = one(*split[0])
    for cut in split[1:]:
        gain = gain * one(*cut)
    return gain


def bell_draw(rng, extent, width, bound, cuts=(), kind=jnp.bfloat16):
    values = jax.random.normal(rng, extent, jnp.float32) * width
    if len(cuts) > 0:
        values = block_scale(rng, extent, cuts, -0.22, 0.18) * values
    return jnp.clip(values, min=-bound, max=bound).astype(kind)


def setup_inputs(seed: int = 0) -> dict:
    arg_keys = jax.random.split(jax.random.key(seed), 10)
    leaf_solution = bell_draw(arg_keys[0], (DEV_ALL * LB, R, P_SIZE), 1.0, 6.0, ((0, 256),))
    leaf_panels = bell_draw(arg_keys[1], (DEV_ALL * LB, 3, NT, P_SIZE, P_SIZE), (P_SIZE * LB * NT) ** -0.5, 0.09375, ((0, 256),))
    leaf_rows = draw_leaf_rows(jax.random.fold_in(arg_keys[9], 71), 0)
    sep_panels = bell_draw(arg_keys[3], (DEV_ALL, 3, NT, P_SIZE, P_SIZE), (P_SIZE * NT) ** -0.5, 0.25, ((0, 256),))
    sep_rows = draw_sep_rows(jax.random.fold_in(arg_keys[9], 71), 0)
    right_sides = bell_draw(arg_keys[5], (3, DEV_ALL, R, P_SIZE), 1.0, 6.0, ((1, 256),))
    inverse_low = bell_draw(arg_keys[6], (DEV_ALL, SEP_BLOCKS * P_SIZE, P_SIZE), (SEP_BLOCKS * P_SIZE) ** -0.5, 0.09375, ((0, 256),))
    inverse_mid = bell_draw(arg_keys[7], (DEV_ALL, 2 * SEP_BLOCKS * P_SIZE, P_SIZE), (2 * SEP_BLOCKS * P_SIZE) ** -0.5, 0.0625, ((0, 256),))
    inverse_top = bell_draw(arg_keys[8], (DEV_ALL, 4 * SEP_BLOCKS * P_SIZE, P_SIZE), (4 * SEP_BLOCKS * P_SIZE) ** -0.5, 0.046875, ((0, 256),))
    return dict(leaf_solution=leaf_solution, leaf_panels=leaf_panels, leaf_rows=leaf_rows, sep_panels=sep_panels, sep_rows=sep_rows, right_sides=right_sides, inverse_low=inverse_low, inverse_mid=inverse_mid, inverse_top=inverse_top)


def leaf_terms(leaf_solution, leaf_panels, leaf_rows):
    total = jnp.zeros((3, DEV_ALL, R, P_SIZE), jnp.float32)

    def one(index, total):
        device = index.astype(jnp.int32)
        values = lax.dynamic_slice_in_dim(leaf_solution, device * LB, LB, 0).astype(jnp.float32)
        panels = lax.dynamic_slice_in_dim(leaf_panels, device * LB, LB, 0).astype(jnp.float32)
        rows = lax.dynamic_slice_in_dim(leaf_rows, device * LB, LB, 0)
        terms = jnp.einsum("brp,bltpq->bltrq", values, panels)
        for level in range(3):
            span = SEP_BLOCKS * 2 ** level
            target = (device // span) * span + rows[:, level, :]
            total = total.at[level, target.reshape(-1)].add(terms[:, level].reshape(-1, R, P_SIZE))
        return total

    return lax.fori_loop(0, DEV_ALL, one, total)


def sep_terms(values, panels, rows, target_level):
    span = SEP_BLOCKS * 2 ** target_level
    terms = jnp.einsum("drp,dtpq->dtrq", values.astype(jnp.float32), panels.astype(jnp.float32))
    base = (jnp.arange(DEV_ALL, dtype=jnp.int32) // span) * span
    target = base[:, None] + rows
    total = jnp.zeros((DEV_ALL, R, P_SIZE), jnp.float32)
    return total.at[target.reshape(-1)].add(terms.reshape(-1, R, P_SIZE))


def settle(resid, inverse, level):
    span = SEP_BLOCKS * 2 ** level
    seps = resid.reshape(DEV_ALL // span, span, R, P_SIZE).transpose(0, 2, 1, 3).reshape(DEV_ALL // span, R, span * P_SIZE)

    def one(device):
        return jnp.dot(seps[device // span], inverse[device], preferred_element_type=jnp.float32)

    return lax.map(one, jnp.arange(DEV_ALL, dtype=jnp.int32)).astype(jnp.bfloat16)


def reference(leaf_solution, leaf_panels, leaf_rows, sep_panels, sep_rows, right_sides, inverse_low, inverse_mid, inverse_top):
    leaf = leaf_terms(leaf_solution, leaf_panels, leaf_rows)
    resid = (right_sides[0].astype(jnp.float32) - leaf[0]).astype(jnp.bfloat16)
    first = settle(resid, inverse_low, 0)
    low_mid = sep_terms(first, sep_panels[:, 0], sep_rows[:, 0], 1)
    low_top = sep_terms(first, sep_panels[:, 1], sep_rows[:, 1], 2)
    resid = (right_sides[1].astype(jnp.float32) - (leaf[1] + low_mid)).astype(jnp.bfloat16)
    second = settle(resid, inverse_mid, 1)
    mid_top = sep_terms(second, sep_panels[:, 2], sep_rows[:, 2], 2)
    resid = (right_sides[2].astype(jnp.float32) - (leaf[2] + low_top + mid_top)).astype(jnp.bfloat16)
    third = settle(resid, inverse_top, 2)
    return jnp.stack([first, second, third])
```

```python
import functools

import jax
import jax.numpy as jnp
from jax import lax
from jax.experimental import pallas as pl
from jax.experimental.pallas import tpu as pltpu
from jax.sharding import PartitionSpec as P

ALONG_X = 4
DEPTH = 8
BF16 = jnp.bfloat16
F32 = jnp.float32
WHOLE = pl.BlockSpec(memory_space=pltpu.VMEM)
SCALARS = pl.BlockSpec(memory_space=pltpu.SMEM)
PARAMS = pltpu.CompilerParams(vmem_limit_bytes=40 * 2**20)


def slot(entry, place):
    x = place[0]
    z = lax.rem(entry, DEPTH)
    step = (lax.div(entry, DEPTH) + (ALONG_X - x)) & (ALONG_X - 1)
    return lax.rem(step, ALONG_X) * DEPTH + z


def slot_at(entry, place, level):
    members = ALONG_X * DEPTH
    inner = slot(lax.rem(entry, members), place)
    group = lax.div(entry, members)
    core = (group & 1) ^ place[1]
    if level == 0:
        return inner
    if level == 1:
        return core * members + inner
    high = (lax.div(group, 2) & 1) ^ place[2]
    return core * (2 * members) + high * members + inner


def leaf_kernel(level, place, rows, values, panels, out, total):
    blocks = out.shape[0]
    count, targets = panels.shape[0], panels.shape[2]

    @pl.loop(0, blocks // 8)
    def _(i):
        total[pl.ds(i * 8, 8)] = jnp.zeros((8, *total.shape[1:]), F32)

    for k in range(count):
        value = values[k]
        for t in range(targets):
            at = slot_at(rows[k * 12 + level * 4 + t], place, level)
            total[at] += jnp.dot(value, panels[k, 0, t], preferred_element_type=F32)

    @pl.loop(0, blocks // 8)
    def _(i):
        out[pl.ds(i * 8, 8)] = total[pl.ds(i * 8, 8)].astype(BF16)


def leaf_sums(level, place, rows, values, panels):
    count, levels, targets, p, q = panels.shape
    height = values.shape[1]
    blocks = ALONG_X * DEPTH * 2**level
    return pl.pallas_call(
        functools.partial(leaf_kernel, level),
        grid=(1,),
        in_specs=[
            SCALARS,
            SCALARS,
            pl.BlockSpec((count, height, p), lambda i: (0, 0, 0)),
            pl.BlockSpec((count, 1, targets, p, q), lambda i: (0, level, 0, 0, 0)),
        ],
        out_specs=pl.BlockSpec((blocks, height, q), lambda i: (0, 0, 0)),
        out_shape=jax.ShapeDtypeStruct((blocks, height, q), BF16),
        scratch_shapes=[pltpu.VMEM((blocks, height, q), F32)],
        compiler_params=PARAMS,
        cost_estimate=pl.CostEstimate(
            flops=2 * count * targets * height * p * q,
            bytes_accessed=2 * count * targets * p * q + 2 * blocks * height * q,
            transcendentals=0,
        ),
        name=f"leaf{level}",
    )(place, rows, values, panels)


def partial_kernel(sets, place, p0, p1, p2, p3, *refs):
    weights, outs = refs[:sets], refs[sets:]
    sums = [None] * sets
    depth = DEPTH * 128
    for k, part in enumerate((p0, p1, p2, p3)):
        lhs = jnp.concatenate([part[z] for z in range(DEPTH)], axis=1)
        start = pl.multiple_of(((place[0] + ALONG_X - k) & (ALONG_X - 1)) * depth, depth)
        for s in range(sets):
            term = jnp.dot(lhs, weights[s][0, pl.ds(start, depth), :], preferred_element_type=F32)
            sums[s] = term if sums[s] is None else sums[s] + term
    for s in range(sets):
        outs[s][...] = sums[s].astype(outs[s].dtype)


def partials(place, parts, inverse, others, kind):
    rows, columns = ALONG_X * DEPTH * 128, inverse.shape[-1]
    height = parts[0].shape[1]
    sets = 1 + len(others)
    fixed = lambda *dims: pl.BlockSpec(dims, lambda i, q: (0,) * len(dims))
    return pl.pallas_call(
        functools.partial(partial_kernel, sets),
        grid_spec=pltpu.PrefetchScalarGridSpec(
            num_scalar_prefetch=1,
            grid=(1,),
            in_specs=[fixed(*parts[0].shape)] * 4
            + [pl.BlockSpec((1, rows, columns), lambda i, q: (0, q[3] if sets > 1 else 0, 0))]
            + [fixed(1, rows, columns)] * (sets - 1),
            out_specs=[fixed(height, columns)] * sets,
        ),
        out_shape=[jax.ShapeDtypeStruct((height, columns), kind)] * sets,
        compiler_params=PARAMS,
        cost_estimate=pl.CostEstimate(
            flops=2 * sets * height * rows * columns,
            bytes_accessed=2 * sets * rows * columns,
            transcendentals=0,
        ),
        name=f"settle{sets}",
    )(place, *parts, inverse, *others)


def add_kernel(level, pair, place, rows, value, panels, base, keep, send):
    half = keep.shape[0]

    @pl.loop(0, half // 8)
    def _(i):
        keep[pl.ds(i * 8, 8)] = base[pl.ds(i * 8, 8)]
        send[pl.ds(i * 8, 8)] = base[pl.ds(half + i * 8, 8)]

    lhs = value[...]
    for t in range(panels.shape[2]):
        at = slot_at(rows[pair * 4 + t], place, level)
        term = jnp.dot(lhs, panels[0, 0, t], preferred_element_type=F32)

        @pl.when(at < half)
        def _():
            keep[at] = (keep[at].astype(F32) + term).astype(BF16)

        @pl.when(at >= half)
        def _():
            send[at - half] = (send[at - half].astype(F32) + term).astype(BF16)


def add_terms(level, pair, place, rows, value, panels, base):
    blocks, height, columns = base.shape
    targets, p = panels.shape[2:4]
    half = jax.ShapeDtypeStruct((blocks // 2, height, columns), BF16)
    fixed = lambda *dims: pl.BlockSpec(dims, lambda i: (0,) * len(dims))
    return pl.pallas_call(
        functools.partial(add_kernel, level, pair),
        grid=(1,),
        in_specs=[
            SCALARS,
            SCALARS,
            fixed(height, p),
            pl.BlockSpec((1, 1, targets, p, columns), lambda i: (0, pair, 0, 0, 0)),
            fixed(*base.shape),
        ],
        out_specs=[fixed(*half.shape)] * 2,
        out_shape=[half, half],
        compiler_params=PARAMS,
        cost_estimate=pl.CostEstimate(
            flops=2 * targets * height * p * columns,
            bytes_accessed=4 * blocks * height * columns,
            transcendentals=0,
        ),
        name=f"add{level}",
    )(place, rows, value, panels, base)


def pieces_kernel(parts, a, b, *outs):
    each = a.shape[0] // parts

    for k in range(parts):

        @pl.loop(0, each // 8)
        def _(i):
            at = pl.ds(k * each + i * 8, 8)
            outs[k][pl.ds(i * 8, 8)] = (a[at].astype(F32) + b[at].astype(F32)).astype(BF16)


def sum_in_pieces(a, b, parts):
    piece = jax.ShapeDtypeStruct((a.shape[0] // parts, *a.shape[1:]), BF16)
    return pl.pallas_call(
        functools.partial(pieces_kernel, parts),
        in_specs=[WHOLE] * 2,
        out_specs=[WHOLE] * parts,
        out_shape=[piece] * parts,
        compiler_params=PARAMS,
        cost_estimate=pl.CostEstimate(flops=a.size, bytes_accessed=6 * a.size, transcendentals=0),
        name=f"pieces{parts}",
    )(a, b)


def terms_kernel(mine, other, panels, out, solution):
    solved = (mine[...] + other[...]).astype(BF16)
    solution[...] = solved
    for t in range(panels.shape[2]):
        out[t] = jnp.dot(solved, panels[0, 0, t], preferred_element_type=F32).astype(BF16)


def solve_and_terms(mine, other, panels, pair):
    height, columns = mine.shape
    targets, p = panels.shape[2:4]
    fixed = lambda *dims: pl.BlockSpec(dims, lambda i: (0,) * len(dims))
    return pl.pallas_call(
        terms_kernel,
        grid=(1,),
        in_specs=[
            fixed(height, columns),
            fixed(height, columns),
            pl.BlockSpec((1, 1, targets, p, columns), lambda i: (0, pair, 0, 0, 0)),
        ],
        out_specs=[fixed(targets, height, columns), fixed(height, columns)],
        out_shape=[
            jax.ShapeDtypeStruct((targets, height, columns), BF16),
            jax.ShapeDtypeStruct((height, columns), BF16),
        ],
        compiler_params=PARAMS,
        cost_estimate=pl.CostEstimate(
            flops=2 * targets * height * p * columns,
            bytes_accessed=4 * targets * p * columns,
            transcendentals=0,
        ),
        name="terms",
    )(mine, other, panels)


def merge_kernel(place, rows, a, b, *refs):
    terms, outs, total = refs[:4], refs[4:8], refs[8]
    blocks = a.shape[0]
    members = ALONG_X * DEPTH

    @pl.loop(0, blocks // 8)
    def _(i):
        at = pl.ds(i * 8, 8)
        total[at] = a[at].astype(F32) + b[at].astype(F32)

    for source, term in enumerate(terms):
        for t in range(term.shape[0]):
            entry = rows[source * 4 + t]

            @pl.when(lax.div(entry, members) == place[3])
            def _():
                at = slot(lax.rem(entry, members), place)
                total[at] += term[t].astype(F32)

    for k in range(ALONG_X):
        outs[k][...] = total[pl.ds(k * DEPTH, DEPTH)].astype(BF16)


def merge(place, rows, a, b, terms):
    piece = jax.ShapeDtypeStruct((DEPTH, *a.shape[1:]), BF16)
    return pl.pallas_call(
        merge_kernel,
        in_specs=[SCALARS] * 2 + [WHOLE] * 6,
        out_specs=[WHOLE] * ALONG_X,
        out_shape=[piece] * ALONG_X,
        scratch_shapes=[pltpu.VMEM(a.shape, F32)],
        compiler_params=PARAMS,
        cost_estimate=pl.CostEstimate(flops=a.size, bytes_accessed=6 * a.size, transcendentals=0),
        name="merge",
    )(place, rows, a, b, *terms)


def along_x(value, step):
    pairs = [
        (x * DEPTH + z, (x + step) % ALONG_X * DEPTH + z)
        for x in range(ALONG_X)
        for z in range(DEPTH)
    ]
    return lax.ppermute(value, "member", pairs)


def swapped(value, mask):
    return lax.ppermute(value, "group", [(g, g ^ mask) for g in range(lax.axis_size("group"))])


def over_z(pieces):
    groups = [[x * DEPTH + z for z in range(DEPTH)] for x in range(ALONG_X)]
    return lax.all_to_all(pieces, "member", 0, 0, axis_index_groups=groups, tiled=True)


def collect(pieces, right):
    arrived = [along_x(pieces[k], k) for k in (2, 1, 3)]
    total = pieces[0].astype(F32)
    for part in arrived:
        total = total + part.astype(F32)
    summed = over_z(total.astype(BF16))
    return (right.astype(F32) - summed.astype(F32).sum(axis=0)).astype(BF16)


def gather(resid):
    own = over_z(jnp.broadcast_to(resid[None], (DEPTH, *resid.shape)))
    far = along_x(own, 2)
    near = [along_x(own, k) for k in (1, 3)]
    return own, near[0], far, near[1]


def on_device(
    leaf_solution,
    leaf_panels,
    leaf_rows,
    sep_panels,
    sep_rows,
    right_sides,
    inverse_low,
    inverse_mid,
    inverse_top,
):
    group = lax.axis_index("group").astype(jnp.int32)
    member = lax.axis_index("member").astype(jnp.int32)
    core, high = group & 1, group >> 1 & 1
    quarter = group & 3
    x = member // DEPTH
    place_mid = jnp.stack([x, core, high, core])
    place = jnp.stack([x, core, high, quarter])
    rows = leaf_rows.reshape(-1)
    source = sep_rows.reshape(-1)
    span = ALONG_X * DEPTH * inverse_low.shape[-1]

    def turned(inverse, count, at):
        return lax.dynamic_slice_in_dim(inverse, at * span, span, 1)

    mid_other = swapped(turned(inverse_mid, 2, core ^ 1), 1)
    top_others = [swapped(turned(inverse_top, 4, quarter ^ mask), mask) for mask in (1, 2, 3)]
    rows_mine = source[8:12]
    rows_high = swapped(rows_mine, 2)
    rows_two = jnp.concatenate([rows_mine, rows_high])
    rows_all = jnp.concatenate([rows_two, swapped(rows_two, 1)])

    base_low = leaf_sums(0, place, rows, leaf_solution, leaf_panels)
    base_mid = leaf_sums(1, place, rows, leaf_solution, leaf_panels)
    base_top = leaf_sums(2, place, rows, leaf_solution, leaf_panels)

    resid = collect([base_low[k * DEPTH : (k + 1) * DEPTH] for k in range(ALONG_X)], right_sides[0, 0])
    (first,) = partials(place, gather(resid), inverse_low, [], BF16)

    keep, send = add_terms(1, 0, place, source, first, sep_panels, base_mid)
    resid = collect(sum_in_pieces(keep, swapped(send, 1), ALONG_X), right_sides[1, 0])

    keep_top, send_top = add_terms(2, 1, place, source, first, sep_panels, base_top)
    stay, leave = sum_in_pieces(keep_top, swapped(send_top, 1), 2)
    arrived = swapped(leave, 2)

    mine, theirs = partials(place_mid, gather(resid), inverse_mid, [mid_other], F32)
    terms, second = solve_and_terms(mine, swapped(theirs, 1), sep_panels, 2)
    terms_high = swapped(terms, 2)
    terms_core = swapped(terms, 1)
    terms_both = swapped(terms_high, 1)
    pieces = merge(place, rows_all, stay, arrived, [terms, terms_high, terms_core, terms_both])
    resid = collect(pieces, right_sides[2, 0])
    mine, by_core, by_high, by_both = partials(place, gather(resid), inverse_top, top_others, F32)
    pair = swapped(jnp.stack([by_high, by_both]), 2)
    third = (mine + pair[0] + swapped(by_core + pair[1], 1)).astype(BF16)
    return jnp.stack([first, second, third])[:, None]


def solution(mesh):
    placed = (
        P(("group", "member"), None, None),
        P(("group", "member"), None, None, None, None),
        P(("group", "member"), None, None),
        P(("group", "member"), None, None, None, None),
        P(("group", "member"), None, None),
        P(None, ("group", "member"), None, None),
        P(("group", "member"), None, None),
        P(("group", "member"), None, None),
        P(("group", "member"), None, None),
    )
    return jax.shard_map(
        on_device,
        mesh=mesh,
        in_specs=placed,
        out_specs=P(None, ("group", "member"), None, None),
        check_vma=False,
    )
```

```python
import functools

import jax
import jax.numpy as jnp
from jax import lax
from jax.experimental import pallas as pl
from jax.experimental.pallas import tpu as pltpu
from jax.sharding import PartitionSpec as P

ALONG_X = 4
DEPTH = 8
BF16 = jnp.bfloat16
F32 = jnp.float32
WHOLE = pl.BlockSpec(memory_space=pltpu.VMEM)
SCALARS = pl.BlockSpec(memory_space=pltpu.SMEM)
PARAMS = pltpu.CompilerParams(vmem_limit_bytes=20 * 2**20)


def here():
    group = lax.axis_index("group").astype(jnp.int32)
    x = lax.div(lax.axis_index("member").astype(jnp.int32), DEPTH)
    return x, group & 1, lax.shift_right_logical(group, 1) & 1, group & 3


def slot(entry, place):
    x = place[0]
    z = lax.rem(entry, DEPTH)
    step = (lax.div(entry, DEPTH) + (ALONG_X - x)) & (ALONG_X - 1)
    return lax.rem(step, ALONG_X) * DEPTH + z


def slot_at(entry, place, level):
    members = ALONG_X * DEPTH
    inner = slot(lax.rem(entry, members), place)
    group = lax.div(entry, members)
    core = (group & 1) ^ place[1]
    if level == 0:
        return inner
    if level == 1:
        return core * members + inner
    high = (lax.div(group, 2) & 1) ^ place[2]
    return core * (2 * members) + high * members + inner


def leaf_kernel(level, each, rows, values, panels, *refs):
    outs, total = refs[:-1], refs[-1]
    blocks = total.shape[0]
    step = pl.program_id(0)
    place = here()

    @pl.when(step == 0)
    def _():
        @pl.loop(0, blocks // 8)
        def _(i):
            total[pl.ds(i * 8, 8)] = jnp.zeros((8, *total.shape[1:]), F32)

    for k in range(each):
        value = values[k]
        for t in range(panels.shape[2]):
            at = slot_at(rows[level, t, step * each + k], place, level)
            total[at] += jnp.dot(value, panels[k, 0, t], preferred_element_type=F32)

    @pl.when(step == pl.num_programs(0) - 1)
    def _():
        held = blocks // len(outs)
        for k, out in enumerate(outs):

            @pl.loop(0, held // 8)
            def _(i):
                out[pl.ds(i * 8, 8)] = total[pl.ds(k * held + i * 8, 8)].astype(BF16)


def leaf_sums(level, rows, values, panels):
    count, _, targets, p, q = panels.shape
    height = values.shape[1]
    blocks = ALONG_X * DEPTH * 2**level
    each = count // 2 if level == 0 else count
    outs = ALONG_X if level == 0 else 1
    return pl.pallas_call(
        functools.partial(leaf_kernel, level, each),
        grid=(count // each,),
        in_specs=[
            SCALARS,
            pl.BlockSpec((each, height, p), lambda i: (i, 0, 0)),
            pl.BlockSpec((each, 1, targets, p, q), lambda i: (i, level, 0, 0, 0)),
        ],
        out_specs=[pl.BlockSpec((blocks // outs, height, q), lambda i: (0, 0, 0))] * outs,
        out_shape=[jax.ShapeDtypeStruct((blocks // outs, height, q), BF16)] * outs,
        scratch_shapes=[pltpu.VMEM((blocks, height, q), F32)],
        compiler_params=pltpu.CompilerParams(vmem_limit_bytes=61 * 2**20)
        if level == 0
        else PARAMS,
        cost_estimate=pl.CostEstimate(
            flops=2 * count * targets * height * p * q,
            bytes_accessed=2 * count * targets * p * q + 2 * blocks * height * q,
            transcendentals=0,
        ),
    )(rows, values, panels)


def partial_kernel(sets, p0, p1, p2, p3, *refs):
    weights, outs = refs[:sets], refs[sets:]
    place = here()
    first = (0, place[1], 0, place[3])[sets - 1] * (ALONG_X * DEPTH * 128)
    sums = [None] * sets
    depth = DEPTH * 128
    for k, part in enumerate((p0, p1, p2, p3)):
        lhs = jnp.concatenate([part[z] for z in range(DEPTH)], axis=1)
        start = pl.multiple_of(((place[0] + ALONG_X - k) & (ALONG_X - 1)) * depth, depth)
        for s in range(sets):
            at = pl.multiple_of(start + first, depth) if s == 0 else start
            term = jnp.dot(lhs, weights[s][0, pl.ds(at, depth), :], preferred_element_type=F32)
            sums[s] = term if sums[s] is None else sums[s] + term
    for s in range(sets):
        outs[s][...] = sums[s].astype(outs[s].dtype)


def partials(parts, inverse, others, kind):
    rows, columns = ALONG_X * DEPTH * 128, inverse.shape[-1]
    height = parts[0].shape[1]
    sets = 1 + len(others)
    return pl.pallas_call(
        functools.partial(partial_kernel, sets),
        in_specs=[WHOLE] * (4 + sets),
        out_specs=[WHOLE] * sets,
        out_shape=[jax.ShapeDtypeStruct((height, columns), kind)] * sets,
        compiler_params=PARAMS,
        cost_estimate=pl.CostEstimate(
            flops=2 * sets * height * rows * columns,
            bytes_accessed=2 * sets * rows * columns,
            transcendentals=0,
        ),
    )(*parts, inverse, *others)


def add_kernel(level, pair, rows, value, panels, base, keep, send):
    half = keep.shape[0]
    place = here()

    @pl.loop(0, half // 8)
    def _(i):
        keep[pl.ds(i * 8, 8)] = base[pl.ds(i * 8, 8)]
        send[pl.ds(i * 8, 8)] = base[pl.ds(half + i * 8, 8)]

    lhs = value[...]
    for t in range(panels.shape[2]):
        at = slot_at(rows[pair, 0, t], place, level)
        term = jnp.dot(lhs, panels[0, 0, t], preferred_element_type=F32)

        @pl.when(at < half)
        def _():
            keep[at] = (keep[at].astype(F32) + term).astype(BF16)

        @pl.when(at >= half)
        def _():
            send[at - half] = (send[at - half].astype(F32) + term).astype(BF16)


def add_terms(level, pair, rows, value, panels, base):
    blocks, height, columns = base.shape
    targets, p = panels.shape[2:4]
    half = jax.ShapeDtypeStruct((blocks // 2, height, columns), BF16)
    fixed = lambda *dims: pl.BlockSpec(dims, lambda i: (0,) * len(dims))
    return pl.pallas_call(
        functools.partial(add_kernel, level, pair),
        grid=(1,),
        in_specs=[
            SCALARS,
            fixed(height, p),
            pl.BlockSpec((1, 1, targets, p, columns), lambda i: (0, pair, 0, 0, 0)),
            fixed(*base.shape),
        ],
        out_specs=[fixed(*half.shape)] * 2,
        out_shape=[half, half],
        compiler_params=PARAMS,
        cost_estimate=pl.CostEstimate(
            flops=2 * targets * height * p * columns,
            bytes_accessed=4 * blocks * height * columns,
            transcendentals=0,
        ),
    )(rows, value, panels, base)


def pieces_kernel(parts, a, b, *outs):
    each = a.shape[0] // parts

    for k in range(parts):

        @pl.loop(0, each // 8)
        def _(i):
            at = pl.ds(k * each + i * 8, 8)
            outs[k][pl.ds(i * 8, 8)] = (a[at].astype(F32) + b[at].astype(F32)).astype(BF16)


def sum_in_pieces(a, b, parts):
    piece = jax.ShapeDtypeStruct((a.shape[0] // parts, *a.shape[1:]), BF16)
    return pl.pallas_call(
        functools.partial(pieces_kernel, parts),
        in_specs=[WHOLE] * 2,
        out_specs=[WHOLE] * parts,
        out_shape=[piece] * parts,
        compiler_params=PARAMS,
        cost_estimate=pl.CostEstimate(flops=a.size, bytes_accessed=6 * a.size, transcendentals=0),
    )(a, b)


def terms_kernel(mine, other, panels, out, solution):
    solved = (mine[...] + other[...]).astype(BF16)
    solution[...] = solved
    for t in range(panels.shape[2]):
        out[t] = jnp.dot(solved, panels[0, 0, t], preferred_element_type=F32).astype(BF16)


def solve_and_terms(mine, other, panels, pair):
    height, columns = mine.shape
    targets, p = panels.shape[2:4]
    fixed = lambda *dims: pl.BlockSpec(dims, lambda i: (0,) * len(dims))
    return pl.pallas_call(
        terms_kernel,
        grid=(1,),
        in_specs=[
            fixed(height, columns),
            fixed(height, columns),
            pl.BlockSpec((1, 1, targets, p, columns), lambda i: (0, pair, 0, 0, 0)),
        ],
        out_specs=[fixed(targets, height, columns), fixed(height, columns)],
        out_shape=[
            jax.ShapeDtypeStruct((targets, height, columns), BF16),
            jax.ShapeDtypeStruct((height, columns), BF16),
        ],
        compiler_params=PARAMS,
        cost_estimate=pl.CostEstimate(
            flops=2 * targets * height * p * columns,
            bytes_accessed=4 * targets * p * columns,
            transcendentals=0,
        ),
        name="terms",
    )(mine, other, panels)


def merge_kernel(rows, a, b, *refs):
    place = here()
    terms, outs, total = refs[:4], refs[4:8], refs[8]
    blocks = a.shape[0]
    members = ALONG_X * DEPTH

    @pl.loop(0, blocks // 8)
    def _(i):
        at = pl.ds(i * 8, 8)
        total[at] = a[at].astype(F32) + b[at].astype(F32)

    for source, term in enumerate(terms):
        for t in range(term.shape[0]):
            entry = rows[source, t]

            @pl.when(lax.div(entry, members) == place[3])
            def _():
                at = slot(lax.rem(entry, members), place)
                total[at] += term[t].astype(F32)

    for k in range(ALONG_X):
        outs[k][...] = total[pl.ds(k * DEPTH, DEPTH)].astype(BF16)


def merge(rows, a, b, terms):
    piece = jax.ShapeDtypeStruct((DEPTH, *a.shape[1:]), BF16)
    return pl.pallas_call(
        merge_kernel,
        in_specs=[SCALARS] + [WHOLE] * 6,
        out_specs=[WHOLE] * ALONG_X,
        out_shape=[piece] * ALONG_X,
        scratch_shapes=[pltpu.VMEM(a.shape, F32)],
        compiler_params=PARAMS,
        cost_estimate=pl.CostEstimate(flops=a.size, bytes_accessed=6 * a.size, transcendentals=0),
        name="merge",
    )(rows, a, b, *terms)


def along_x(value, step):
    pairs = [
        (x * DEPTH + z, (x + step) % ALONG_X * DEPTH + z)
        for x in range(ALONG_X)
        for z in range(DEPTH)
    ]
    return lax.ppermute(value, "member", pairs)


def swapped(value, mask):
    return lax.ppermute(value, "group", [(g, g ^ mask) for g in range(lax.axis_size("group"))])


def over_z(pieces):
    groups = [[x * DEPTH + z for z in range(DEPTH)] for x in range(ALONG_X)]
    return lax.all_to_all(pieces, "member", 0, 0, axis_index_groups=groups, tiled=True)


def resid_kernel(level, arrived, right, out):
    total = right[level, 0].astype(F32)
    for z in range(DEPTH):
        total = total - arrived[z].astype(F32)
    resid = total.astype(BF16)
    for z in range(DEPTH):
        out[z] = resid


def residual_copies(arrived, right, level):
    return pl.pallas_call(
        functools.partial(resid_kernel, level),
        in_specs=[WHOLE] * 2,
        out_specs=WHOLE,
        out_shape=jax.ShapeDtypeStruct(arrived.shape, BF16),
        compiler_params=PARAMS,
        cost_estimate=pl.CostEstimate(flops=arrived.size, bytes_accessed=4 * arrived.size, transcendentals=0),
    )(arrived, right)


def collect(pieces, right, level):
    arrived = [along_x(pieces[k], k) for k in (2, 1, 3)]
    total = pieces[0].astype(F32)
    for part in arrived:
        total = total + part.astype(F32)
    total = total.astype(BF16)
    return residual_copies(over_z(total), right, level)


def gather(copies):
    own = over_z(copies)
    far = along_x(own, 2)
    near = [along_x(own, k) for k in (1, 3)]
    return own, near[0], far, near[1]


def on_device(
    leaf_solution,
    leaf_panels,
    leaf_rows,
    sep_panels,
    sep_rows,
    right_sides,
    inverse_low,
    inverse_mid,
    inverse_top,
):
    quarter = lax.axis_index("group").astype(jnp.int32) & 3
    rows = leaf_rows.transpose(1, 2, 0)
    source = sep_rows.transpose(1, 0, 2)
    span = ALONG_X * DEPTH * inverse_low.shape[-1]

    def turned(inverse, at):
        return lax.dynamic_slice_in_dim(inverse, at * span, span, 1)

    pieces = leaf_sums(0, rows, leaf_solution, leaf_panels)

    mid_other = swapped(turned(inverse_mid, quarter & 1 ^ 1), 1)
    top_others = []
    for mask in (1, 2, 3):
        top_others.append(swapped(turned(inverse_top, quarter ^ mask), mask))
    rows_mine = source[2]
    rows_high = swapped(rows_mine, 2)
    rows_two = jnp.concatenate([rows_mine, rows_high])
    rows_core = swapped(rows_two, 1)
    rows_all = jnp.concatenate([rows_two, rows_core])

    (base_mid,) = leaf_sums(1, rows, leaf_solution, leaf_panels)
    (base_top,) = leaf_sums(2, rows, leaf_solution, leaf_panels)

    copies = collect(pieces, right_sides, 0)
    (first,) = partials(gather(copies), inverse_low, [], BF16)

    keep, send = add_terms(1, 0, source, first, sep_panels, base_mid)
    copies = collect(sum_in_pieces(keep, swapped(send, 1), ALONG_X), right_sides, 1)

    keep_top, send_top = add_terms(2, 1, source, first, sep_panels, base_top)
    stay, leave = sum_in_pieces(keep_top, swapped(send_top, 1), 2)
    arrived = swapped(leave, 2)

    mine, theirs = partials(gather(copies), inverse_mid, [mid_other], F32)
    terms, second = solve_and_terms(mine, swapped(theirs, 1), sep_panels, 2)
    terms_high = swapped(terms, 2)
    terms_core = swapped(terms, 1)
    terms_both = swapped(terms_high, 1)
    pieces = merge(rows_all, stay, arrived, [terms, terms_high, terms_core, terms_both])
    copies = collect(pieces, right_sides, 2)
    mine, by_core, by_high, by_both = partials(gather(copies), inverse_top, top_others, F32)
    pair = swapped(jnp.stack([by_high, by_both]), 2)
    third = (mine + pair[0] + swapped(by_core + pair[1], 1)).astype(BF16)
    return jnp.stack([first, second, third])[:, None]


def solution(mesh):
    placed = (
        P(("group", "member"), None, None),
        P(("group", "member"), None, None, None, None),
        P(("group", "member"), None, None),
        P(("group", "member"), None, None, None, None),
        P(("group", "member"), None, None),
        P(None, ("group", "member"), None, None),
        P(("group", "member"), None, None),
        P(("group", "member"), None, None),
        P(("group", "member"), None, None),
    )
    return jax.shard_map(
        on_device,
        mesh=mesh,
        in_specs=placed,
        out_specs=P(None, ("group", "member"), None, None),
        check_vma=False,
    )
```

```python
import functools

import jax
import jax.numpy as jnp
from jax import lax
from jax.experimental import pallas as pl
from jax.experimental.pallas import tpu as pltpu
from jax.sharding import PartitionSpec as P

ALONG_X = 4
DEPTH = 8
BF16 = jnp.bfloat16
F32 = jnp.float32
WHOLE = pl.BlockSpec(memory_space=pltpu.VMEM)
SCALARS = pl.BlockSpec(memory_space=pltpu.SMEM)
PARAMS = pltpu.CompilerParams(vmem_limit_bytes=20 * 2**20)


def here():
    group = lax.axis_index("group").astype(jnp.int32)
    x = lax.div(lax.axis_index("member").astype(jnp.int32), DEPTH)
    return x, group & 1, lax.shift_right_logical(group, 1) & 1, group & 3


def slot(entry, place):
    x = place[0]
    z = lax.rem(entry, DEPTH)
    step = (lax.div(entry, DEPTH) + (ALONG_X - x)) & (ALONG_X - 1)
    return lax.rem(step, ALONG_X) * DEPTH + z


def slot_at(entry, place, level):
    members = ALONG_X * DEPTH
    inner = slot(lax.rem(entry, members), place)
    group = lax.div(entry, members)
    core = (group & 1) ^ place[1]
    if level == 0:
        return inner
    if level == 1:
        return core * members + inner
    high = (lax.div(group, 2) & 1) ^ place[2]
    return core * (2 * members) + high * members + inner


def leaf_kernel(level, each, rows, values, panels, *refs):
    outs, total = refs[:-1], refs[-1]
    blocks = total.shape[0]
    step = pl.program_id(0)
    place = here()

    @pl.when(step == 0)
    def _():
        @pl.loop(0, blocks // 8)
        def _(i):
            total[pl.ds(i * 8, 8)] = jnp.zeros((8, *total.shape[1:]), F32)

    for k in range(each):
        value = values[k]
        for t in range(panels.shape[2]):
            at = slot_at(rows[level, t, step * each + k], place, level)
            total[at] += jnp.dot(value, panels[k, 0, t], preferred_element_type=F32)

    @pl.when(step == pl.num_programs(0) - 1)
    def _():
        held = blocks // len(outs)
        for k, out in enumerate(outs):

            @pl.loop(0, held // 8)
            def _(i):
                out[pl.ds(i * 8, 8)] = total[pl.ds(k * held + i * 8, 8)].astype(BF16)


def leaf_sums(level, rows, values, panels):
    count, _, targets, p, q = panels.shape
    height = values.shape[1]
    blocks = ALONG_X * DEPTH * 2**level
    each = count // 2 if level == 0 else count
    outs = ALONG_X if level == 0 else 1
    return pl.pallas_call(
        functools.partial(leaf_kernel, level, each),
        grid=(count // each,),
        in_specs=[
            SCALARS,
            pl.BlockSpec((each, height, p), lambda i: (i, 0, 0)),
            pl.BlockSpec((each, 1, targets, p, q), lambda i: (i, level, 0, 0, 0)),
        ],
        out_specs=[pl.BlockSpec((blocks // outs, height, q), lambda i: (0, 0, 0))] * outs,
        out_shape=[jax.ShapeDtypeStruct((blocks // outs, height, q), BF16)] * outs,
        scratch_shapes=[pltpu.VMEM((blocks, height, q), F32)],
        compiler_params=pltpu.CompilerParams(vmem_limit_bytes=52 * 2**20)
        if level == 0
        else PARAMS,
        cost_estimate=pl.CostEstimate(
            flops=2 * count * targets * height * p * q,
            bytes_accessed=2 * count * targets * p * q + 2 * blocks * height * q,
            transcendentals=0,
        ),
    )(rows, values, panels)


def partial_kernel(sets, p0, p1, p2, p3, *refs):
    weights, outs = refs[:sets], refs[sets:]
    place = here()
    first = (0, place[1], 0, place[3])[sets - 1] * (ALONG_X * DEPTH * 128)
    sums = [None] * sets
    depth = DEPTH * 128
    for k, part in enumerate((p0, p1, p2, p3)):
        lhs = jnp.concatenate([part[z] for z in range(DEPTH)], axis=1)
        start = pl.multiple_of(((place[0] + ALONG_X - k) & (ALONG_X - 1)) * depth, depth)
        for s in range(sets):
            at = pl.multiple_of(start + first, depth) if s == 0 else start
            term = jnp.dot(lhs, weights[s][0, pl.ds(at, depth), :], preferred_element_type=F32)
            sums[s] = term if sums[s] is None else sums[s] + term
    for s in range(sets):
        outs[s][...] = sums[s].astype(outs[s].dtype)


def partials(parts, inverse, others, kind):
    rows, columns = ALONG_X * DEPTH * 128, inverse.shape[-1]
    height = parts[0].shape[1]
    sets = 1 + len(others)
    return pl.pallas_call(
        functools.partial(partial_kernel, sets),
        in_specs=[WHOLE] * (4 + sets),
        out_specs=[WHOLE] * sets,
        out_shape=[jax.ShapeDtypeStruct((height, columns), kind)] * sets,
        compiler_params=PARAMS,
        cost_estimate=pl.CostEstimate(
            flops=2 * sets * height * rows * columns,
            bytes_accessed=2 * sets * rows * columns,
            transcendentals=0,
        ),
    )(*parts, inverse, *others)


def add_kernel(level, pair, rows, value, panels, base, keep, send):
    half = keep.shape[0]
    place = here()

    @pl.loop(0, half // 8)
    def _(i):
        keep[pl.ds(i * 8, 8)] = base[pl.ds(i * 8, 8)]
        send[pl.ds(i * 8, 8)] = base[pl.ds(half + i * 8, 8)]

    lhs = value[...]
    for t in range(panels.shape[2]):
        at = slot_at(rows[pair, 0, t], place, level)
        term = jnp.dot(lhs, panels[0, 0, t], preferred_element_type=F32)

        @pl.when(at < half)
        def _():
            keep[at] = (keep[at].astype(F32) + term).astype(BF16)

        @pl.when(at >= half)
        def _():
            send[at - half] = (send[at - half].astype(F32) + term).astype(BF16)


def add_terms(level, pair, rows, value, panels, base):
    blocks, height, columns = base.shape
    targets, p = panels.shape[2:4]
    half = jax.ShapeDtypeStruct((blocks // 2, height, columns), BF16)
    fixed = lambda *dims: pl.BlockSpec(dims, lambda i: (0,) * len(dims))
    return pl.pallas_call(
        functools.partial(add_kernel, level, pair),
        grid=(1,),
        in_specs=[
            SCALARS,
            fixed(height, p),
            pl.BlockSpec((1, 1, targets, p, columns), lambda i: (0, pair, 0, 0, 0)),
            fixed(*base.shape),
        ],
        out_specs=[fixed(*half.shape)] * 2,
        out_shape=[half, half],
        compiler_params=PARAMS,
        cost_estimate=pl.CostEstimate(
            flops=2 * targets * height * p * columns,
            bytes_accessed=4 * blocks * height * columns,
            transcendentals=0,
        ),
    )(rows, value, panels, base)


def pieces_kernel(parts, a, b, *outs):
    each = a.shape[0] // parts

    for k in range(parts):

        @pl.loop(0, each // 8)
        def _(i):
            at = pl.ds(k * each + i * 8, 8)
            outs[k][pl.ds(i * 8, 8)] = (a[at].astype(F32) + b[at].astype(F32)).astype(BF16)


def sum_in_pieces(a, b, parts):
    piece = jax.ShapeDtypeStruct((a.shape[0] // parts, *a.shape[1:]), BF16)
    return pl.pallas_call(
        functools.partial(pieces_kernel, parts),
        in_specs=[WHOLE] * 2,
        out_specs=[WHOLE] * parts,
        out_shape=[piece] * parts,
        compiler_params=PARAMS,
        cost_estimate=pl.CostEstimate(flops=a.size, bytes_accessed=6 * a.size, transcendentals=0),
    )(a, b)


def terms_kernel(mine, other, panels, out, solution):
    solved = (mine[...] + other[...]).astype(BF16)
    solution[...] = solved
    for t in range(panels.shape[2]):
        out[t] = jnp.dot(solved, panels[0, 0, t], preferred_element_type=F32).astype(BF16)


def solve_and_terms(mine, other, panels, pair):
    height, columns = mine.shape
    targets, p = panels.shape[2:4]
    fixed = lambda *dims: pl.BlockSpec(dims, lambda i: (0,) * len(dims))
    return pl.pallas_call(
        terms_kernel,
        grid=(1,),
        in_specs=[
            fixed(height, columns),
            fixed(height, columns),
            pl.BlockSpec((1, 1, targets, p, columns), lambda i: (0, pair, 0, 0, 0)),
        ],
        out_specs=[fixed(targets, height, columns), fixed(height, columns)],
        out_shape=[
            jax.ShapeDtypeStruct((targets, height, columns), BF16),
            jax.ShapeDtypeStruct((height, columns), BF16),
        ],
        compiler_params=PARAMS,
        cost_estimate=pl.CostEstimate(
            flops=2 * targets * height * p * columns,
            bytes_accessed=4 * targets * p * columns,
            transcendentals=0,
        ),
        name="terms",
    )(mine, other, panels)


def merge_kernel(*refs):
    place = here()
    rows, (a, b), terms, outs, total = refs[:4], refs[4:6], refs[6:10], refs[10:14], refs[14]
    blocks = a.shape[0]
    members = ALONG_X * DEPTH

    @pl.loop(0, blocks // 8)
    def _(i):
        at = pl.ds(i * 8, 8)
        total[at] = a[at].astype(F32) + b[at].astype(F32)

    for source, term in enumerate(terms):
        for t in range(term.shape[0]):
            entry = rows[source][2, 0, t]

            @pl.when(lax.div(entry, members) == place[3])
            def _():
                at = slot(lax.rem(entry, members), place)
                total[at] += term[t].astype(F32)

    for k in range(ALONG_X):
        outs[k][...] = total[pl.ds(k * DEPTH, DEPTH)].astype(BF16)


def merge(rows, a, b, terms):
    piece = jax.ShapeDtypeStruct((DEPTH, *a.shape[1:]), BF16)
    return pl.pallas_call(
        merge_kernel,
        in_specs=[SCALARS] * 4 + [WHOLE] * 6,
        out_specs=[WHOLE] * ALONG_X,
        out_shape=[piece] * ALONG_X,
        scratch_shapes=[pltpu.VMEM(a.shape, F32)],
        compiler_params=PARAMS,
        cost_estimate=pl.CostEstimate(flops=a.size, bytes_accessed=6 * a.size, transcendentals=0),
        name="merge",
    )(*rows, a, b, *terms)


def finish_kernel(first, second, a, b, c, d, out):
    out[0, 0] = first[...]
    out[1, 0] = second[...]
    out[2, 0] = (a[...] + b[...] + c[...] + d[...]).astype(BF16)


def finish(*args):
    return pl.pallas_call(
        finish_kernel,
        in_specs=[WHOLE] * 6,
        out_specs=WHOLE,
        out_shape=jax.ShapeDtypeStruct((3, 1, *args[0].shape), BF16),
        compiler_params=PARAMS,
        name="finish",
    )(*args)


def along_x(value, step):
    pairs = [
        (x * DEPTH + z, (x + step) % ALONG_X * DEPTH + z)
        for x in range(ALONG_X)
        for z in range(DEPTH)
    ]
    return lax.ppermute(value, "member", pairs)


def swapped(value, mask):
    return lax.ppermute(value, "group", [(g, g ^ mask) for g in range(lax.axis_size("group"))])


def over_z(pieces):
    groups = [[x * DEPTH + z for z in range(DEPTH)] for x in range(ALONG_X)]
    return lax.all_to_all(pieces, "member", 0, 0, axis_index_groups=groups, tiled=True)


def resid_kernel(level, arrived, right, out):
    total = right[level, 0].astype(F32)
    for z in range(DEPTH):
        total = total - arrived[z].astype(F32)
    resid = total.astype(BF16)
    for z in range(DEPTH):
        out[z] = resid


def residual_copies(arrived, right, level):
    return pl.pallas_call(
        functools.partial(resid_kernel, level),
        in_specs=[WHOLE] * 2,
        out_specs=WHOLE,
        out_shape=jax.ShapeDtypeStruct(arrived.shape, BF16),
        compiler_params=PARAMS,
        cost_estimate=pl.CostEstimate(flops=arrived.size, bytes_accessed=4 * arrived.size, transcendentals=0),
    )(arrived, right)


def collect(pieces, right, level):
    arrived = [along_x(pieces[k], k) for k in (2, 1, 3)]
    total = pieces[0].astype(F32)
    for part in arrived:
        total = total + part.astype(F32)
    total = total.astype(BF16)
    summed = over_z(total)
    return residual_copies(summed, right, level)


def gather(copies):
    own = over_z(copies)
    far = along_x(own, 2)
    near = [along_x(own, k) for k in (1, 3)]
    return own, near[0], far, near[1]


def on_device(
    leaf_solution,
    leaf_panels,
    leaf_rows,
    sep_panels,
    sep_rows,
    right_sides,
    inverse_low,
    inverse_mid,
    inverse_top,
):
    quarter = lax.axis_index("group").astype(jnp.int32) & 3
    rows = leaf_rows.transpose(1, 2, 0)
    source = sep_rows.transpose(1, 0, 2)
    span = ALONG_X * DEPTH * inverse_low.shape[-1]

    def turned(inverse, at):
        return lax.dynamic_slice_in_dim(inverse, at * span, span, 1)

    pieces = leaf_sums(0, rows, leaf_solution, leaf_panels)

    mid_other = swapped(turned(inverse_mid, quarter & 1 ^ 1), 1)
    top_others = []
    for mask in (1, 2, 3):
        top_others.append(swapped(turned(inverse_top, quarter ^ mask), mask))
    rows_all = [source]
    for mask in (2, 1, 3):
        rows_all.append(swapped(source, mask))

    (base_mid,) = leaf_sums(1, rows, leaf_solution, leaf_panels)
    (base_top,) = leaf_sums(2, rows, leaf_solution, leaf_panels)

    copies = collect(pieces, right_sides, 0)
    (first,) = partials(gather(copies), inverse_low, [], BF16)

    keep, send = add_terms(1, 0, source, first, sep_panels, base_mid)
    copies = collect(sum_in_pieces(keep, swapped(send, 1), ALONG_X), right_sides, 1)

    keep_top, send_top = add_terms(2, 1, source, first, sep_panels, base_top)
    stay, leave = sum_in_pieces(keep_top, swapped(send_top, 1), 2)
    arrived = swapped(leave, 2)

    mine, theirs = partials(gather(copies), inverse_mid, [mid_other], F32)
    terms, second = solve_and_terms(mine, swapped(theirs, 1), sep_panels, 2)
    terms_high = swapped(terms, 2)
    terms_core = swapped(terms, 1)
    terms_both = swapped(terms_high, 1)
    pieces = merge(rows_all, stay, arrived, [terms, terms_high, terms_core, terms_both])
    pieces, top_others = lax.optimization_barrier((pieces, top_others))
    copies = collect(pieces, right_sides, 2)
    mine, by_core, by_high, by_both = partials(gather(copies), inverse_top, top_others, F32)
    arrived = [swapped(by_high, 2), swapped(by_both, 3), swapped(by_core, 1)]
    return finish(first, second, mine, *arrived)


def solution(mesh):
    placed = (
        P(("group", "member"), None, None),
        P(("group", "member"), None, None, None, None),
        P(("group", "member"), None, None),
        P(("group", "member"), None, None, None, None),
        P(("group", "member"), None, None),
        P(None, ("group", "member"), None, None),
        P(("group", "member"), None, None),
        P(("group", "member"), None, None),
        P(("group", "member"), None, None),
    )
    return jax.shard_map(
        on_device,
        mesh=mesh,
        in_specs=placed,
        out_specs=P(None, ("group", "member"), None, None),
        check_vma=False,
    )
```
